32 devices in a mesh: heads: 4 (over y, core), blk: 8 (over z, x).
Axes of the slice: x: 2, y: 2, z: 4, core: 2. Of those that a mesh axis runs over, the one named last changes fastest.
Arguments:
- tokens: bfloat16 [4096, 4096], P(('blk', 'heads')), may hold values from -6 to 6
- w_query: bfloat16 [4096, 2048], P('blk', 'heads'), may hold values from -0.75 to 0.75
- key_value_weight: bfloat16 [4096, 2, 512], P('blk', None, 'heads'), may hold values from -0.75 to 0.75
- w_out: bfloat16 [2048, 4096], P(('heads', 'blk')), may hold values from -0.5 to 0.5
- doc_lengths: int32 [16], replicated, may hold values from 1 to 1024, 4096 in all
Outputs:
- attended: bfloat16 [4096, 4096], P(('blk', 'heads'))
The draws below stay inside these ranges and needn't reach their ends.
Inputs may be any that keep to these rules, and one draw needn't show every extreme that they name: `doc_lengths`: the 16 lengths sum to 4096; the longest document has exactly 1024 tokens.
All inputs are finite; a program needn't handle non-finite values.
Results may differ from the reference program's by a relative error of at most 0.012.
Values may be sent and summed in bfloat16 or wider, within the bound.
No kernel may reach another device: no remote copies, remote signals or barrier semaphores. Data moves between devices by JAX's collectives and lax.ppermute only.
A program may use at most 128 MiB of HBM per device.

```python
import math
import jax
import jax.numpy as jnp
import numpy as np
from jax import lax

MODEL_WIDTH = 4096
QUERY_HEADS = 16
KEY_VALUE_HEADS = 4
HEAD_SIZE = 128
NDOC = 16
PACK_TOKENS = 4096
BLOCK_TOKENS = 512
DOC_MAX = 1024
REACH = 2


def shared_weights(key):
    expand_heads = MODEL_WIDTH ** (-0.5)
    base_query = jax.random.truncated_normal(jax.random.fold_in(key, 11), -6.0, 6.0, (MODEL_WIDTH, QUERY_HEADS, HEAD_SIZE), jnp.float32) * expand_heads
    unrotated_keys = jax.random.truncated_normal(jax.random.fold_in(key, 12), -6.0, 6.0, (MODEL_WIDTH, KEY_VALUE_HEADS, HEAD_SIZE), jnp.float32) * expand_heads
    projected_values = jax.random.truncated_normal(jax.random.fold_in(key, 13), -6.0, 6.0, (MODEL_WIDTH, KEY_VALUE_HEADS, HEAD_SIZE), jnp.float32) * expand_heads
    key_matrix = unrotated_keys
    query_weights = base_query
    limit = 48.0 * expand_heads
    query_weights = jnp.clip(query_weights, -limit, limit).reshape(MODEL_WIDTH, QUERY_HEADS * HEAD_SIZE)
    key_value_matrix = jnp.stack([key_matrix.reshape(MODEL_WIDTH, KEY_VALUE_HEADS * HEAD_SIZE), projected_values.reshape(MODEL_WIDTH, KEY_VALUE_HEADS * HEAD_SIZE)], axis=1)
    key_value_matrix = jnp.clip(key_value_matrix, -limit, limit)
    return (query_weights, key_value_matrix)


def draw_w_query(key, part):
    return shared_weights(key)[0].astype(jnp.bfloat16)


def draw_key_value_weight(key, part):
    return shared_weights(key)[1].astype(jnp.bfloat16)


def draw_tokens(key, part):
    own_part = jax.random.normal(jax.random.fold_in(key, 21), (PACK_TOKENS, MODEL_WIDTH), jnp.float32)
    result = own_part
    return jnp.clip(result, -6.0, 6.0).astype(jnp.bfloat16)


def block_scale(own_key, dims, cuts, low, high):
    loudness = 1.0
    for position, blocks in cuts:
        steps = jax.random.uniform(jax.random.fold_in(jax.random.fold_in(own_key, 6), position), (blocks,), jnp.float32, low / len(cuts), high / len(cuts))
        loudness = loudness * jnp.repeat(jnp.exp(steps), dims[position] // blocks).reshape((-1,) + (1,) * (len(dims) - 1 - position))
    return loudness


def split_up(count, total, most, slope):
    weights = [(1 << 20) // math.isqrt(rank ** slope) + 1 for rank in range(2, count + 1)]
    surplus, holding = total - most - (count - 1), [1] * (count - 1)
    while surplus > 0:
        movable = [i for i in range(count - 1) if holding[i] < most]
        pool, budget = sum([weights[i] for i in movable]), surplus
        for i in movable:
            more = min(most - holding[i], max(1, budget * weights[i] // pool), surplus)
            holding[i] = holding[i] + more
            surplus = surplus - more
    return np.array([most] + holding)


def ragged_sizes(key, amount, total, most, slope):
    if amount == 2:
        one = jax.random.randint(key, (), max(1, total - most), min(most, total - 1) + 1)
        return jnp.stack([one, total - one])
    sizes = jnp.asarray(split_up(amount, total, most, slope), jnp.int32)
    twos = (amount - 1) // 2
    source_of, sink = sizes[1:1 + 2 * twos:2], sizes[2:2 + 2 * twos:2]
    room = jnp.minimum(source_of - 1, most - sink)
    passed = jax.random.randint(jax.random.fold_in(key, 1), (twos,), 0, 1 << 20) % (room + 1)
    sizes = sizes.at[1:1 + 2 * twos:2].set(source_of - passed).at[2:2 + 2 * twos:2].set(sink + passed)
    return sizes[jax.random.permutation(jax.random.fold_in(key, 2), amount)]


def scatter_about(stream_key, shape, scale, most, split=(), kind=jnp.bfloat16):
    values = jax.random.normal(stream_key, shape, jnp.float32) * scale
    if len(split) > 0:
        values = block_scale(stream_key, shape, split, -0.22, 0.18) * values
    return jnp.clip(values, min=-most, max=most).astype(kind)


def setup_inputs(seed: int = 0) -> dict:
    keys = jax.random.split(jax.random.key(seed), 6)
    return {
        "tokens": draw_tokens(jax.random.fold_in(keys[5], 71), 0),
        "w_query": draw_w_query(jax.random.fold_in(keys[5], 71), 0),
        "key_value_weight": draw_key_value_weight(jax.random.fold_in(keys[5], 71), 0),
        "w_out": scatter_about(keys[3], (QUERY_HEADS * HEAD_SIZE, MODEL_WIDTH), HEAD_SIZE ** -0.5, 0.5, ((0, 32),)),
        "doc_lengths": ragged_sizes(keys[4], NDOC, PACK_TOKENS, DOC_MAX, 2).astype(jnp.int32),
    }


norm_epsilon = 1e-05
rope_base = 500000.0
masked_score = -1e+30

def locate_documents(positions, doc_lengths):
    ends = jnp.cumsum(doc_lengths).astype(jnp.int32)
    after = positions[:, None] >= ends[None, :]
    ident = lax.optimization_barrier(jnp.sum(after.astype(jnp.int32), axis=1))
    starts = lax.optimization_barrier(jnp.sum(jnp.where(after, doc_lengths[None, :], 0), axis=1)).astype(jnp.int32)
    return (ident, starts)

def apply_rotation(values, relative_offset):
    half = values.shape[-1] // 2
    freqs = jnp.power(rope_base, -2.0 * jnp.arange(half, dtype=jnp.float32) / values.shape[-1])
    angle = relative_offset.astype(jnp.float32)[:, None] * freqs[None, :]
    cosine = jnp.cos(angle)[:, None, :]
    sine = jnp.sin(angle)[:, None, :]
    first = values[..., :half]
    second = values[..., half:]
    return jnp.concatenate([first * cosine - second * sine, second * cosine + first * sine], axis=-1)

def reference(tokens, w_query, key_value_weight, w_out, doc_lengths):
    values = tokens.astype(jnp.float32)
    normalized_input = (values * lax.rsqrt(lax.optimization_barrier(jnp.mean(values * values, axis=1, keepdims=True)) + norm_epsilon)).astype(jnp.bfloat16)
    query_raw = jnp.dot(normalized_input, w_query, preferred_element_type=jnp.float32)
    key_value_projected = jnp.dot(normalized_input, key_value_weight.reshape(MODEL_WIDTH, 2 * KEY_VALUE_HEADS * HEAD_SIZE), preferred_element_type=jnp.float32)
    positions = jnp.arange(PACK_TOKENS, dtype=jnp.int32)
    ident, starts = locate_documents(positions, doc_lengths)
    relative_offset = positions - starts
    query_rows = apply_rotation(query_raw.reshape(PACK_TOKENS, QUERY_HEADS, HEAD_SIZE), relative_offset).astype(jnp.bfloat16)
    rotated_keys = apply_rotation(key_value_projected[:, :KEY_VALUE_HEADS * HEAD_SIZE].reshape(PACK_TOKENS, KEY_VALUE_HEADS, HEAD_SIZE), relative_offset).astype(jnp.bfloat16)
    value_rows = key_value_projected[:, KEY_VALUE_HEADS * HEAD_SIZE:].reshape(PACK_TOKENS, KEY_VALUE_HEADS, HEAD_SIZE).astype(jnp.bfloat16)
    front_offset = REACH * BLOCK_TOKENS
    window = (REACH + 1) * BLOCK_TOKENS
    padded_key_rows = jnp.concatenate([jnp.zeros((front_offset, KEY_VALUE_HEADS, HEAD_SIZE), jnp.bfloat16), rotated_keys], axis=0)
    padded_value_rows = jnp.concatenate([jnp.zeros((front_offset, KEY_VALUE_HEADS, HEAD_SIZE), jnp.bfloat16), value_rows], axis=0)
    head_group = QUERY_HEADS // KEY_VALUE_HEADS
    scale = HEAD_SIZE ** (-0.5)

    def one_block(block_index):
        leading_row = (block_index * BLOCK_TOKENS).astype(jnp.int32)
        query_block_rows = lax.dynamic_slice_in_dim(query_rows, leading_row, BLOCK_TOKENS, 0).reshape(BLOCK_TOKENS, KEY_VALUE_HEADS, head_group, HEAD_SIZE).astype(jnp.float32)
        key_block = lax.dynamic_slice_in_dim(padded_key_rows, leading_row, window, 0).astype(jnp.float32)
        value_block = lax.dynamic_slice_in_dim(padded_value_rows, leading_row, window, 0).astype(jnp.float32)
        query_pos = leading_row + jnp.arange(BLOCK_TOKENS, dtype=jnp.int32)
        key_pos = leading_row - front_offset + jnp.arange(window, dtype=jnp.int32)
        query_doc, unused_q = locate_documents(query_pos, doc_lengths)
        key_doc, unused_k = locate_documents(key_pos, doc_lengths)
        keep = (key_pos[None, :] >= 0) & (key_pos[None, :] <= query_pos[:, None]) & (key_doc[None, :] == query_doc[:, None])
        scores = jnp.einsum('qhgd,khd->hgqk', query_block_rows, key_block) * scale
        scores = jnp.where(keep, scores, masked_score)
        highest = lax.optimization_barrier(jnp.max(scores, axis=-1, keepdims=True))
        probs = jnp.where(keep, jnp.exp(scores - highest), 0.0)
        totals = lax.optimization_barrier(jnp.sum(probs, axis=-1))
        probs_b = lax.optimization_barrier(probs.astype(jnp.bfloat16))
        mixed = jnp.einsum('hgqk,khd->hgqd', probs_b.astype(jnp.float32), value_block)
        mixed = mixed / totals[..., None]
        return mixed.transpose(2, 0, 1, 3).reshape(BLOCK_TOKENS, QUERY_HEADS * HEAD_SIZE).astype(jnp.bfloat16)
    mixed_all = lax.map(one_block, jnp.arange(PACK_TOKENS // BLOCK_TOKENS, dtype=jnp.int32)).reshape(PACK_TOKENS, QUERY_HEADS * HEAD_SIZE)
    return jnp.dot(mixed_all, w_out, preferred_element_type=jnp.float32).astype(jnp.bfloat16)
```

```python
import functools

import jax
import jax.numpy as jnp
from jax import lax
from jax.experimental import pallas as pl
from jax.experimental.pallas import tpu as pltpu
from jax.sharding import Mesh
from jax.sharding import PartitionSpec as P

HEAD_SIZE = 128
norm_epsilon = 1e-05
rope_base = 500000.0
masked_score = -1e30
PAIR = 2
OUT_CHUNKS = 4


SWAP = [(0, 1), (1, 0)]


def ranks_of(doc_lengths, positions):
    ends = jnp.cumsum(doc_lengths)
    after = positions[:, None] >= ends[None, :]
    return jnp.sum(jnp.where(after, doc_lengths[None, :], 0), axis=1)


def attend(order_ref, q_ref, cos_ref, sin_ref, low_ref, *refs, planes, heads, stripes, rows):
    kv_refs, (out_ref, k_all, v_all) = refs[: 2 * planes], refs[2 * planes :]
    core = order_ref[heads]
    half = HEAD_SIZE // 2
    span = stripes * PAIR * rows
    for plane in range(planes):
        for which in range(2):
            source = kv_refs[2 * plane + which]
            side = core if which == 0 else 1 - core
            for stripe in range(stripes):
                place = plane * span + (order_ref[heads + 1 + stripe] * PAIR + side) * rows
                place = pl.multiple_of(place, rows)
                taken = slice(stripe * rows, (stripe + 1) * rows)
                k_all[pl.ds(place, rows), :] = source[taken, :HEAD_SIZE]
                v_all[pl.ds(place, rows), :] = source[taken, HEAD_SIZE:]
    width = (planes - 1) * span + PAIR * rows
    scale = HEAD_SIZE ** (-0.5)

    def one_stripe(stripe, unused):
        taken = pl.ds(pl.multiple_of(stripe * rows, rows), rows)
        index = order_ref[heads + 1 + stripe]
        base = pl.multiple_of(index * PAIR * rows, PAIR * rows)
        keys = k_all[pl.ds(base, width), :]
        values = v_all[pl.ds(base, width), :]
        cosine, sine = cos_ref[taken, :], sin_ref[taken, :]
        key_pos = base + lax.broadcasted_iota(jnp.int32, (rows, width), 1)
        own_pos = (planes - 1) * span + base + core * rows
        own_pos = own_pos + lax.broadcasted_iota(jnp.int32, (rows, width), 0)
        keep = (key_pos >= low_ref[taken, :1]) & (key_pos <= own_pos)
        for head in range(heads):
            lane = pl.multiple_of(order_ref[head] * HEAD_SIZE, HEAD_SIZE)
            raw = q_ref[taken, pl.ds(lane, HEAD_SIZE)]
            query = (raw * cosine + pltpu.roll(raw, half, 1) * sine).astype(jnp.bfloat16)
            score = lax.dot_general(
                query, keys, (((1,), (1,)), ((), ())), preferred_element_type=jnp.float32
            )
            score = jnp.where(keep, score * scale, masked_score)
            high = jnp.max(score, axis=1, keepdims=True)
            probs = jnp.exp(score - high)
            total = jnp.sum(probs, axis=1, keepdims=True)
            mixed = jnp.dot(
                probs.astype(jnp.bfloat16), values, preferred_element_type=jnp.float32
            )
            out_ref[taken, head * HEAD_SIZE : (head + 1) * HEAD_SIZE] = (mixed / total).astype(
                jnp.bfloat16
            )
        return unused

    lax.fori_loop(0, stripes, one_stripe, 0)


def on_device(tokens, w_query, key_value_weight, w_out, doc_lengths):
    z, x, y, core = (lax.axis_index(name) for name in ("z", "x", "y", "core"))
    depth = lax.axis_size("z")
    rows, features = tokens.shape
    stripes = PAIR * PAIR
    block = w_query.shape[0]
    query_cols = w_query.shape[1]
    heads = query_cols // HEAD_SIZE
    line = depth == 4 and heads == depth
    if line:
        far = jnp.where(z < 2, 2, 1)
        order = jnp.stack([z, z ^ 1, far, far ^ 1]).astype(jnp.int32)
    else:
        order = jnp.arange(depth, dtype=jnp.int32)

    def exchange(part):
        other = lax.ppermute(part, ("core", "x"), [(1, 2), (2, 1)])
        return jnp.where(x == core, part, other)

    def gather(part):
        if not line:
            held = [lax.all_gather(part, "z", axis=0, tiled=False)]
        else:
            near = lax.ppermute(part, "z", [(0, 1), (1, 0), (2, 3), (3, 2)])
            pair = jnp.stack([part, near])
            middle = lax.ppermute(pair, "z", [(1, 2), (2, 1)])
            end = lax.ppermute(middle, "z", [(1, 0), (2, 3)])
            held = [pair, jnp.where((z == 1) | (z == 2), middle, end)]
        return held, [lax.ppermute(piece, "core", SWAP) for piece in held]

    values = tokens.astype(jnp.float32)
    normed = (
        values * lax.rsqrt(jnp.mean(values * values, axis=1, keepdims=True) + norm_epsilon)
    ).astype(jnp.bfloat16)
    spots = [order[i] * PAIR + side for side in (core, 1 - core) for i in range(depth)]
    normed = jnp.concatenate(
        [lax.dynamic_slice_in_dim(normed, spot * block, block, 1) for spot in spots], axis=1
    )
    by_y = lax.ppermute(normed, "y", SWAP)
    by_x = lax.ppermute(normed, "x", SWAP)
    by_both = lax.ppermute(by_x, "y", SWAP)
    block_input = jnp.concatenate([normed, by_y, by_x, by_both], axis=0)
    stripe_index = jnp.stack([(x ^ dx) * PAIR + (y ^ dy) for dx in (0, 1) for dy in (0, 1)])
    stripe_index = stripe_index.astype(jnp.int32)

    def project(pieces):
        total, at = None, 0
        for piece in pieces[0] + pieces[1]:
            count = piece.shape[0] * piece.shape[1]
            term = jnp.dot(
                block_input[:, at : at + count],
                piece.reshape(count, -1),
                preferred_element_type=jnp.float32,
            )
            total, at = (term if total is None else total + term), at + count
        return total

    keyval_own = exchange(key_value_weight.reshape(block, -1))
    query_own = exchange(w_query)
    out_own = exchange(w_out)
    keyval_weights = gather(keyval_own)
    query_weights = gather(query_own)

    span = stripes * PAIR * rows
    planes = depth // 4 + 1
    positions = (
        z * span
        + (stripe_index[:, None] * PAIR + core) * rows
        + jnp.arange(rows, dtype=jnp.int32)[None, :]
    ).reshape(-1)
    starts = ranks_of(doc_lengths, positions)
    half = HEAD_SIZE // 2
    freqs = jnp.power(rope_base, -2.0 * jnp.arange(half, dtype=jnp.float32) / HEAD_SIZE)
    angle = (positions - starts).astype(jnp.float32)[:, None] * freqs[None, :]
    cosine, sine = jnp.cos(angle), jnp.sin(angle)
    cosine = jnp.concatenate([cosine, cosine], axis=1)
    sine = jnp.concatenate([-sine, sine], axis=1)
    low = starts - (z - (planes - 1)) * span
    low = jnp.broadcast_to(low[:, None], (low.shape[0], HEAD_SIZE))

    keyval = project(keyval_weights)
    key_raw = keyval[:, :HEAD_SIZE]
    turned = jnp.concatenate([key_raw[:, half:], key_raw[:, :half]], axis=1)
    keys = key_raw * cosine + turned * sine
    rest = keyval[:, HEAD_SIZE:]
    keyval = jnp.concatenate([keys, rest], axis=1).astype(jnp.bfloat16)
    held = []
    for distance in range(planes - 1, -1, -1):
        own = keyval
        if distance:
            pairs = [(i, i + distance) for i in range(depth - distance)]
            own = lax.ppermute(keyval, "z", pairs)
        held += [own, lax.ppermute(own, "core", SWAP)]

    query_raw = project(query_weights)
    scalars = jnp.concatenate([order[:heads] if line else jnp.arange(heads, dtype=jnp.int32),
                               core[None].astype(jnp.int32), stripe_index])
    count = stripes * rows
    mixed = pl.pallas_call(
        functools.partial(attend, planes=planes, heads=heads, stripes=stripes, rows=rows),
        out_shape=jax.ShapeDtypeStruct((count, query_cols), jnp.bfloat16),
        in_specs=[pl.BlockSpec(memory_space=pltpu.SMEM)]
        + [pl.BlockSpec(memory_space=pltpu.VMEM)] * (4 + 2 * planes),
        out_specs=pl.BlockSpec(memory_space=pltpu.VMEM),
        scratch_shapes=[pltpu.VMEM((planes * span, HEAD_SIZE), jnp.bfloat16)] * 2,
        compiler_params=pltpu.CompilerParams(vmem_limit_bytes=60000 * 1024),
        cost_estimate=pl.CostEstimate(
            flops=8 * count * query_cols * planes * span // 2, bytes_accessed=8 << 20, transcendentals=0
        ),
        name="attend",
    )(scalars, query_raw, cosine, sine, low, *held)

    width = w_out.shape[1] // OUT_CHUNKS
    outs = []
    for chunk in range(OUT_CHUNKS):
        own, other = gather(out_own[:, chunk * width : (chunk + 1) * width])
        per = w_out.shape[0]
        mine = jnp.concatenate(own, axis=0)
        theirs = jnp.concatenate(other, axis=0)
        first = jnp.where(core == 0, mine, theirs)
        second = jnp.where(core == 0, theirs, mine)
        weights = jnp.stack([first, second], axis=1).reshape(2 * depth * per, width)
        share = jnp.dot(mixed, weights, preferred_element_type=jnp.float32).astype(jnp.bfloat16)
        share = share.reshape(PAIR, PAIR, rows, width)
        if chunk % 2 == 0:
            got = lax.ppermute(share[:, 1], "y", SWAP)
            kept = share[:, 0].astype(jnp.float32) + got.astype(jnp.float32)
            kept = kept.astype(jnp.bfloat16)
            got = lax.ppermute(kept[1], "x", SWAP)
        else:
            got = lax.ppermute(share[1], "x", SWAP)
            kept = share[0].astype(jnp.float32) + got.astype(jnp.float32)
            kept = kept.astype(jnp.bfloat16)
            got = lax.ppermute(kept[1], "y", SWAP)
        outs.append((kept[0].astype(jnp.float32) + got.astype(jnp.float32)).astype(jnp.bfloat16))
    return jnp.concatenate(outs, axis=1)


def solution(mesh):
    groups, blocks = mesh.shape["heads"], mesh.shape["blk"]
    fine = Mesh(
        mesh.devices.reshape(groups // PAIR, PAIR, blocks // PAIR, PAIR),
        ("y", "core", "z", "x"),
    )
    return jax.shard_map(
        on_device,
        mesh=fine,
        in_specs=(
            P(("z", "x", "y", "core"), None),
            P(("z", "x"), ("y", "core")),
            P(("z", "x"), None, ("y", "core")),
            P(("y", "core", "z", "x"), None),
            P(),
        ),
        out_specs=P(("z", "x", "y", "core"), None),
        check_vma=False,
    )
```

```python
import functools

import jax
import jax.numpy as jnp
from jax import lax
from jax.experimental import pallas as pl
from jax.experimental.pallas import tpu as pltpu
from jax.sharding import Mesh
from jax.sharding import PartitionSpec as P

HEAD_SIZE = 128
norm_epsilon = 1e-05
rope_base = 500000.0
masked_score = -1e30
LOG2_E = 1.4426950408889634
PAIR = 2
OUT_CHUNKS = 4
FIRST_SUM = ("yx", "yx", "yx", "yx")
QUERY_CHUNKS = 2


SWAP = [(0, 1), (1, 0)]
BESIDE = [(0, 1), (1, 0), (2, 3), (3, 2)]


def ranks_of(doc_lengths, positions):
    ends = jnp.cumsum(doc_lengths)
    after = positions[:, None] >= ends[None, :]
    return jnp.sum(jnp.where(after, doc_lengths[None, :], 0), axis=1)


def normalise(spot_ref, token_ref, *out_refs, block, aligned):
    features = token_ref.shape[1]
    first = 0
    for out_ref in out_refs:
        taken = slice(first, first + out_ref.shape[0])
        first += out_ref.shape[0]
        squares = jnp.zeros((out_ref.shape[0], 1), jnp.float32)
        for i in range(features // block):
            part = token_ref[taken, i * block : (i + 1) * block].astype(jnp.float32)
            squares += jnp.sum(part * part, axis=1, keepdims=True)
        factor = lax.rsqrt(squares * (1.0 / features) + norm_epsilon)
        if not aligned:
            out_ref[...] = (token_ref[taken, :].astype(jnp.float32) * factor).astype(jnp.bfloat16)
            continue
        for i in range(features // block):
            at = pl.multiple_of(spot_ref[i] * block, block)
            part = token_ref[taken, pl.ds(at, block)].astype(jnp.float32)
            out_ref[:, i * block : (i + 1) * block] = (part * factor).astype(jnp.bfloat16)


def product(token_refs, weight_refs):
    total, at = None, 0
    for ref in weight_refs:
        count, columns = ref.shape[0] * ref.shape[1], ref.shape[2]
        part = jnp.concatenate([tokens[:, at : at + count] for tokens in token_refs], axis=0)
        term = jnp.dot(part, ref[...].reshape(count, columns), preferred_element_type=jnp.float32)
        total, at = (term if total is None else total + term), at + count
    return total


def keys_values(cos_ref, sin_ref, *refs, held):
    token_refs, weight_refs, out_ref = refs[:held], refs[held:-1], refs[-1]
    both = product(token_refs, weight_refs)
    raw = both[:, :HEAD_SIZE]
    turned = raw * cos_ref[...] + pltpu.roll(raw, HEAD_SIZE // 2, 1) * sin_ref[...]
    out_ref[:, :HEAD_SIZE] = turned.astype(jnp.bfloat16)
    out_ref[:, HEAD_SIZE:] = both[:, HEAD_SIZE:].astype(jnp.bfloat16)


def attend(index_ref, cos_ref, sin_ref, low_ref, *refs, planes, held, heads, stripes, rows):
    out_ref, q_all, k_all, v_all = refs[-4:]
    kv_refs = refs[-4 - 2 * planes : -4]
    q_all[...] = product(refs[:held], refs[held : -4 - 2 * planes])
    core = index_ref[0]
    half = HEAD_SIZE // 2
    span = stripes * PAIR * rows
    for plane in range(planes):
        for which in range(2):
            source = kv_refs[2 * plane + which]
            side = core if which == 0 else 1 - core
            for stripe in range(stripes):
                place = plane * span + (index_ref[1 + stripe] * PAIR + side) * rows
                place = pl.multiple_of(place, rows)
                taken = slice(stripe * rows, (stripe + 1) * rows)
                k_all[pl.ds(place, rows), :] = source[taken, :HEAD_SIZE]
                v_all[pl.ds(place, rows), :] = source[taken, HEAD_SIZE:]
    width = (planes - 1) * span + PAIR * rows
    scale = HEAD_SIZE ** (-0.5) * LOG2_E

    def one_stripe(stripe, unused):
        taken = pl.ds(pl.multiple_of(stripe * rows, rows), rows)
        index = index_ref[1 + stripe]
        base = pl.multiple_of(index * PAIR * rows, PAIR * rows)
        keys = k_all[pl.ds(base, width), :]
        values = v_all[pl.ds(base, width), :]
        cosine, sine = cos_ref[taken, :], sin_ref[taken, :]
        key_pos = base + lax.broadcasted_iota(jnp.int32, (rows, width), 1)
        own_pos = (planes - 1) * span + base + core * rows
        own_pos = own_pos + lax.broadcasted_iota(jnp.int32, (rows, width), 0)
        keep = (key_pos >= low_ref[taken, :1]) & (key_pos <= own_pos)
        bias = jnp.where(keep, 0.0, masked_score)
        for head in range(heads):
            lanes = slice(head * HEAD_SIZE, (head + 1) * HEAD_SIZE)
            raw = q_all[taken, lanes]
            query = (raw * cosine + pltpu.roll(raw, half, 1) * sine).astype(jnp.bfloat16)
            score = lax.dot_general(
                query, keys, (((1,), (1,)), ((), ())), preferred_element_type=jnp.float32
            )
            score = score * scale + bias
            probs = jnp.exp2(score - jnp.max(score, axis=1, keepdims=True))
            total = jnp.sum(probs, axis=1, keepdims=True)
            mixed = jnp.dot(
                probs.astype(jnp.bfloat16), values, preferred_element_type=jnp.float32
            )
            out_ref[taken, lanes] = (mixed / total).astype(jnp.bfloat16)
        return unused

    lax.fori_loop(0, stripes, one_stripe, 0, unroll=2)


def share_out(index_ref, *refs, parts, axes, inner):
    count = 2 * len(axes) + 1
    mixed_refs, pieces, (*out_refs, weights) = refs[:parts], refs[parts:-count], refs[-count:]
    core = index_ref[0]
    for which, piece in enumerate(pieces):
        first = index_ref[1] if which % 2 == 0 else PAIR - index_ref[1]
        side = core if which < 2 else 1 - core
        per = piece.shape[1]
        for i in range(piece.shape[0]):
            row = pl.multiple_of(((first + i) * PAIR + side) * per, per)
            skip = 0 if piece.shape[2] == weights.shape[1] else inner
            weights[pl.ds(row, per), :] = piece[i, :, skip : skip + weights.shape[1]]
    mixed = jnp.concatenate([ref[...] for ref in mixed_refs], axis=1)
    columns = weights.shape[1] // len(axes)
    rows = mixed.shape[0] // (PAIR * PAIR)
    tile = min(columns, 2 * HEAD_SIZE)
    for part, axis in enumerate(axes):
        keep_ref, send_ref = out_refs[2 * part : 2 * part + 2]
        for at in range(0, columns, tile):
            start = part * columns + at
            share = jnp.dot(
                mixed, weights[:, start : start + tile], preferred_element_type=jnp.float32
            ).astype(jnp.bfloat16)
            for dx in range(PAIR):
                for dy in range(PAIR):
                    piece = share[(dx * PAIR + dy) * rows : (dx * PAIR + dy + 1) * rows]
                    sent, place = (dy, dx) if axis == "y" else (dx, dy)
                    (send_ref if sent else keep_ref)[place, :, at : at + tile] = piece


def last_sum(*refs):
    *parts, out_ref = refs
    at = 0
    for kept_ref, got_ref in zip(parts[::2], parts[1::2]):
        total = kept_ref[0].astype(jnp.float32) + got_ref[...].astype(jnp.float32)
        out_ref[:, at : at + total.shape[1]] = total.astype(jnp.bfloat16)
        at += total.shape[1]


VMEM = pl.BlockSpec(memory_space=pltpu.VMEM)
SMEM = pl.BlockSpec(memory_space=pltpu.SMEM)


def kernel(body, out_shape, operands, scalars=0, scratch=(), flops=0, **static):
    return pl.pallas_call(
        functools.partial(body, **static),
        out_shape=out_shape,
        in_specs=[SMEM] * scalars + [VMEM] * (len(operands) - scalars),
        out_specs=jax.tree.map(lambda unused: VMEM, out_shape),
        scratch_shapes=scratch,
        compiler_params=pltpu.CompilerParams(vmem_limit_bytes=40000 * 1024),
        cost_estimate=pl.CostEstimate(
            flops=flops, bytes_accessed=1 << 20, transcendentals=0
        ),
    )(*operands)


def on_device(tokens, w_query, key_value_weight, w_out, doc_lengths):
    z, x, y, core = (lax.axis_index(name) for name in ("z", "x", "y", "core"))
    depth = lax.axis_size("z")
    rows, features = tokens.shape
    stripes = PAIR * PAIR
    block = w_query.shape[0]
    line = depth == 4

    def exchange(part):
        other = lax.ppermute(part, ("core", "x"), [(1, 2), (2, 1)])
        return jnp.where(x == core, part, other)

    def near_of(part):
        near = lax.ppermute(part, "z", BESIDE)
        even = z % 2 == 0
        return jnp.stack([jnp.where(even, part, near), jnp.where(even, near, part)])

    def middle_of(pair):
        return lax.ppermute(pair, "z", [(1, 2), (2, 1)])

    def far_of(middle):
        end = lax.ppermute(middle, "z", [(1, 0), (2, 3)])
        return jnp.where((z == 1) | (z == 2), middle, end)

    def gathered(part):
        held = lax.all_gather(part, "z", axis=0, tiled=False)
        return held, lax.ppermute(held, "core", SWAP)

    spots = jnp.arange(PAIR * depth, dtype=jnp.int32)
    flip = z // 2 * 2 if line else 0
    spots = ((spots % depth) ^ flip) * PAIR + ((spots // depth) ^ core)
    cut = rows * 5 // 8
    normed = kernel(
        normalise,
        [jax.ShapeDtypeStruct((count, features), jnp.bfloat16) for count in (cut, rows - cut)],
        (spots, tokens),
        scalars=1,
        flops=1 << 30,
        block=block,
        aligned=block % HEAD_SIZE == 0,
    )
    if block % HEAD_SIZE:
        normed = [
            jnp.take(part.reshape(len(part), -1, block), spots, axis=1).reshape(part.shape)
            for part in normed
        ]
    by_y = [lax.ppermute(normed[i], "y", SWAP) for i in range(2)]
    by_x = [lax.ppermute(normed[i], "x", SWAP) for i in range(2)]
    by_both = [lax.ppermute(by_x[0], "y", SWAP), lax.ppermute(by_y[1], "x", SWAP)]
    block_input = (*normed, *by_y, *by_x, *by_both)
    stripe_index = jnp.arange(stripes, dtype=jnp.int32) ^ (x * PAIR + y)

    keyval_own = exchange(key_value_weight).reshape(block, -1)
    query_own = exchange(w_query)
    out_own = exchange(w_out)
    if line:
        pair = near_of(keyval_own)
        far = far_of(middle_of(pair))
        keyval_weights = [
            pair, far, lax.ppermute(pair, "core", SWAP), lax.ppermute(far, "core", SWAP)
        ]
        pairs = jnp.split(near_of(query_own), QUERY_CHUNKS, axis=2)
        query_weights = []
        for pair in pairs:
            far = far_of(middle_of(pair))
            query_weights.append([
                pair, far, lax.ppermute(pair, "core", SWAP), lax.ppermute(far, "core", SWAP)
            ])
    else:
        keyval_weights = gathered(keyval_own)
        query_weights = [gathered(part) for part in jnp.split(query_own, QUERY_CHUNKS, axis=1)]

    span = stripes * PAIR * rows
    planes = depth // 4 + 1
    positions = (
        z * span
        + (stripe_index[:, None] * PAIR + core) * rows
        + jnp.arange(rows, dtype=jnp.int32)[None, :]
    ).reshape(-1)
    starts = ranks_of(doc_lengths, positions)
    half = HEAD_SIZE // 2
    freqs = jnp.power(rope_base, -2.0 * jnp.arange(half, dtype=jnp.float32) / HEAD_SIZE)
    angle = (positions - starts).astype(jnp.float32)[:, None] * freqs[None, :]
    cosine, sine = jnp.cos(angle), jnp.sin(angle)
    cosine = jnp.concatenate([cosine, cosine], axis=1)
    sine = jnp.concatenate([-sine, sine], axis=1)
    low = starts - (z - (planes - 1)) * span
    low = jnp.broadcast_to(low[:, None], (low.shape[0], HEAD_SIZE))

    count = stripes * rows
    keyval = kernel(
        keys_values,
        jax.ShapeDtypeStruct((count, 2 * HEAD_SIZE), jnp.bfloat16),
        (cosine, sine, *block_input, *keyval_weights),
        flops=4 * count * features * HEAD_SIZE,
        held=len(block_input),
    )
    held = []
    for distance in range(planes - 1, -1, -1):
        own = keyval
        if distance:
            steps = [(i, i + distance) for i in range(depth - distance)]
            own = lax.ppermute(keyval, "z", steps)
        held += [own, lax.ppermute(own, "core", SWAP)]

    scalars = jnp.arange(-1, stripes, dtype=jnp.int32)
    scalars = jnp.where(scalars < 0, core, scalars ^ (x * PAIR + y))
    mixed = []
    for weights in query_weights:
        columns = weights[0].shape[-1]
        mixed.append(
            kernel(
                attend,
                jax.ShapeDtypeStruct((count, columns), jnp.bfloat16),
                (scalars, cosine, sine, low, *block_input, *weights, *held),
                scalars=1,
                scratch=[pltpu.VMEM((count, columns), jnp.float32)]
                + [pltpu.VMEM((planes * span, HEAD_SIZE), jnp.bfloat16)] * 2,
                flops=2 * count * columns * (features + 2 * planes * span),
                planes=planes,
                held=len(block_input),
                heads=columns // HEAD_SIZE,
                stripes=stripes,
                rows=rows,
            )
        )
    place = jnp.stack([core, z // 2 * 2]).astype(jnp.int32)

    width = w_out.shape[1] // OUT_CHUNKS
    per = w_out.shape[0]
    if line:
        halves = []
        near = lax.ppermute(out_own, "z", BESIDE)
        half = w_out.shape[1] // 2
        for at in (0, half):
            pair = (out_own[:, at : at + half], near[:, at : at + half])
            even = z % 2 == 0
            pair = [jnp.where(even, pair[0], pair[1]), jnp.where(even, pair[1], pair[0])]
            pair = lax.optimization_barrier(jnp.stack(pair))
            pair_c = lax.ppermute(pair, "core", SWAP)
            middle = middle_of(pair)
            cuts = [middle[:, :, at : at + width] for at in range(0, half, width)]
            halves.append((pair, pair_c, lax.optimization_barrier(cuts)))
    outs = []
    for chunk in range(OUT_CHUNKS):
        cols = slice(chunk * width, (chunk + 1) * width)
        axes = FIRST_SUM[chunk]
        if line:
            pair, pair_c, middle = halves[chunk * 2 // OUT_CHUNKS]
            inner = chunk % (OUT_CHUNKS // 2)
            far = far_of(middle[inner])
            far_c = lax.ppermute(far, "core", SWAP)
            shares = kernel(
                share_out,
                [jax.ShapeDtypeStruct((PAIR, rows, width // len(axes)), jnp.bfloat16)]
                * (2 * len(axes)),
                (place, *mixed, pair, far, pair_c, far_c),
                scalars=1,
                scratch=[pltpu.VMEM((2 * depth * per, width), jnp.bfloat16)],
                flops=2 * count * 2 * depth * per * width,
                parts=len(mixed),
                axes=axes,
                inner=inner * width,
            )
        else:
            mine, theirs = gathered(out_own[:, cols])
            weights = jnp.stack(
                [jnp.where(core == 0, mine, theirs), jnp.where(core == 0, theirs, mine)], axis=1
            ).reshape(2 * depth * per, width)
            share = jnp.dot(
                jnp.concatenate(mixed, axis=1), weights, preferred_element_type=jnp.float32
            ).astype(jnp.bfloat16)
            share = share.reshape(PAIR, PAIR, rows, len(axes), width // len(axes))
            shares = [
                share[:, i, :, part] if axis == "y" else share[i, :, :, part]
                for part, axis in enumerate(axes)
                for i in range(PAIR)
            ]
        for part, axis in enumerate(axes):
            kept, sent = shares[2 * part : 2 * part + 2]
            got = lax.ppermute(sent, axis, SWAP)
            kept = kept.astype(jnp.float32) + got.astype(jnp.float32)
            kept = kept.astype(jnp.bfloat16)
            other = "x" if axis == "y" else "y"
            outs += [kept, lax.ppermute(kept[1], other, SWAP)]
    return kernel(last_sum, jax.ShapeDtypeStruct((rows, w_out.shape[1]), jnp.bfloat16), outs)


def solution(mesh):
    groups, blocks = mesh.shape["heads"], mesh.shape["blk"]
    depth = blocks // PAIR
    fine = Mesh(
        mesh.devices.reshape(groups // PAIR, PAIR, depth, PAIR),
        ("y", "core", "z", "x"),
    )
    return jax.shard_map(
        on_device,
        mesh=fine,
        in_specs=(
            P(("z", "x", "y", "core"), None),
            P(("z", "x"), ("y", "core")),
            P(("z", "x"), None, ("y", "core")),
            P(("y", "core", "z", "x"), None),
            P(),
        ),
        out_specs=P(("z", "x", "y", "core"), None),
        check_vma=False,
    )
```

```python
import functools

import jax
import jax.numpy as jnp
from jax import lax
from jax.experimental import pallas as pl
from jax.experimental.pallas import tpu as pltpu
from jax.sharding import Mesh
from jax.sharding import PartitionSpec as P

HEAD_SIZE = 128
norm_epsilon = 1e-05
rope_base = 500000.0
masked_score = -1e30
LOG2_E = 1.4426950408889634
PAIR = 2
OUT_CHUNKS = 4
FIRST_SUM = ("yx", "yx", "yx", "yx")
QUERY_CHUNKS = 2


SWAP = [(0, 1), (1, 0)]
BESIDE = [(0, 1), (1, 0), (2, 3), (3, 2)]


def ranks_of(doc_lengths, positions):
    ends = jnp.cumsum(doc_lengths)
    after = positions[:, None] >= ends[None, :]
    return jnp.sum(jnp.where(after, doc_lengths[None, :], 0), axis=1)


def normalise(spot_ref, token_ref, *out_refs, block, aligned):
    features = token_ref.shape[1]
    first = 0
    for out_ref in out_refs:
        taken = slice(first, first + out_ref.shape[0])
        first += out_ref.shape[0]
        squares = jnp.zeros((out_ref.shape[0], 1), jnp.float32)
        for i in range(features // block):
            part = token_ref[taken, i * block : (i + 1) * block].astype(jnp.float32)
            squares += jnp.sum(part * part, axis=1, keepdims=True)
        factor = lax.rsqrt(squares * (1.0 / features) + norm_epsilon)
        if not aligned:
            out_ref[...] = (token_ref[taken, :].astype(jnp.float32) * factor).astype(jnp.bfloat16)
            continue
        for i in range(features // block):
            at = pl.multiple_of(spot_ref[i] * block, block)
            part = token_ref[taken, pl.ds(at, block)].astype(jnp.float32)
            out_ref[:, i * block : (i + 1) * block] = (part * factor).astype(jnp.bfloat16)


def product(token_refs, weight_refs):
    total, at = None, 0
    for ref in weight_refs:
        count, columns = ref.shape[0] * ref.shape[1], ref.shape[2]
        part = jnp.concatenate([tokens[:, at : at + count] for tokens in token_refs], axis=0)
        term = jnp.dot(part, ref[...].reshape(count, columns), preferred_element_type=jnp.float32)
        total, at = (term if total is None else total + term), at + count
    return total


def keys_values(cos_ref, sin_ref, *refs, held):
    token_refs, weight_refs, out_ref = refs[:held], refs[held:-1], refs[-1]
    both = product(token_refs, weight_refs)
    raw = both[:, :HEAD_SIZE]
    turned = raw * cos_ref[...] + pltpu.roll(raw, HEAD_SIZE // 2, 1) * sin_ref[...]
    out_ref[:, :HEAD_SIZE] = turned.astype(jnp.bfloat16)
    out_ref[:, HEAD_SIZE:] = both[:, HEAD_SIZE:].astype(jnp.bfloat16)


def attend(index_ref, cos_ref, sin_ref, low_ref, *refs, planes, held, heads, stripes, rows):
    out_ref, q_all, k_all, v_all = refs[-4:]
    kv_refs = refs[-4 - 2 * planes : -4]
    q_all[...] = product(refs[:held], refs[held : -4 - 2 * planes])
    core = index_ref[0]
    half = HEAD_SIZE // 2
    span = stripes * PAIR * rows
    for plane in range(planes):
        for which in range(2):
            source = kv_refs[2 * plane + which]
            side = core if which == 0 else 1 - core
            for stripe in range(stripes):
                place = plane * span + (index_ref[1 + stripe] * PAIR + side) * rows
                place = pl.multiple_of(place, rows)
                taken = slice(stripe * rows, (stripe + 1) * rows)
                k_all[pl.ds(place, rows), :] = source[taken, :HEAD_SIZE]
                v_all[pl.ds(place, rows), :] = source[taken, HEAD_SIZE:]
    width = (planes - 1) * span + PAIR * rows
    scale = HEAD_SIZE ** (-0.5) * LOG2_E

    def one_stripe(stripe, unused):
        taken = pl.ds(pl.multiple_of(stripe * rows, rows), rows)
        index = index_ref[1 + stripe]
        base = pl.multiple_of(index * PAIR * rows, PAIR * rows)
        keys = k_all[pl.ds(base, width), :]
        values = v_all[pl.ds(base, width), :]
        cosine, sine = cos_ref[taken, :], sin_ref[taken, :]
        key_pos = base + lax.broadcasted_iota(jnp.int32, (rows, width), 1)
        own_pos = (planes - 1) * span + base + core * rows
        own_pos = own_pos + lax.broadcasted_iota(jnp.int32, (rows, width), 0)
        keep = (key_pos >= low_ref[taken, :1]) & (key_pos <= own_pos)
        bias = jnp.where(keep, 0.0, masked_score)
        raw = [q_all[taken, h * HEAD_SIZE : (h + 1) * HEAD_SIZE] for h in range(heads)]
        query = jnp.concatenate(
            [(part * cosine + pltpu.roll(part, half, 1) * sine) for part in raw], axis=0
        ).astype(jnp.bfloat16)
        score = lax.dot_general(
            query, keys, (((1,), (1,)), ((), ())), preferred_element_type=jnp.float32
        )
        score = (score * scale).reshape(heads, rows, width) + bias[None]
        probs = jnp.exp2(score - jnp.max(score, axis=2, keepdims=True))
        total = jnp.sum(probs, axis=2, keepdims=True)
        mixed = jnp.dot(
            probs.reshape(heads * rows, width).astype(jnp.bfloat16),
            values,
            preferred_element_type=jnp.float32,
        ).reshape(heads, rows, HEAD_SIZE)
        mixed = (mixed / total).astype(jnp.bfloat16)
        for h in range(heads):
            out_ref[taken, h * HEAD_SIZE : (h + 1) * HEAD_SIZE] = mixed[h]
        return unused

    lax.fori_loop(0, stripes, one_stripe, 0)


def share_out(index_ref, *refs, parts, axes, inner):
    count = 2 * len(axes) + 1
    mixed_refs, pieces, (*out_refs, weights) = refs[:parts], refs[parts:-count], refs[-count:]
    core = index_ref[0]
    for which, piece in enumerate(pieces):
        first = index_ref[1] if which % 2 == 0 else PAIR - index_ref[1]
        side = core if which < 2 else 1 - core
        per = piece.shape[1]
        for i in range(piece.shape[0]):
            row = pl.multiple_of(((first + i) * PAIR + side) * per, per)
            skip = 0 if piece.shape[2] == weights.shape[1] else inner
            weights[pl.ds(row, per), :] = piece[i, :, skip : skip + weights.shape[1]]
    mixed = jnp.concatenate([ref[...] for ref in mixed_refs], axis=1)
    columns = weights.shape[1] // len(axes)
    rows = mixed.shape[0] // (PAIR * PAIR)
    tile = min(columns, 2 * HEAD_SIZE)
    for part, axis in enumerate(axes):
        keep_ref, send_ref = out_refs[2 * part : 2 * part + 2]
        for at in range(0, columns, tile):
            start = part * columns + at
            share = jnp.dot(
                mixed, weights[:, start : start + tile], preferred_element_type=jnp.float32
            ).astype(jnp.bfloat16)
            for dx in range(PAIR):
                for dy in range(PAIR):
                    piece = share[(dx * PAIR + dy) * rows : (dx * PAIR + dy + 1) * rows]
                    sent, place = (dy, dx) if axis == "y" else (dx, dy)
                    (send_ref if sent else keep_ref)[place, :, at : at + tile] = piece


def last_sum(*refs):
    *parts, out_ref = refs
    at = 0
    for kept_ref, got_ref in zip(parts[::2], parts[1::2]):
        total = kept_ref[0].astype(jnp.float32) + got_ref[...].astype(jnp.float32)
        out_ref[:, at : at + total.shape[1]] = total.astype(jnp.bfloat16)
        at += total.shape[1]


VMEM = pl.BlockSpec(memory_space=pltpu.VMEM)
SMEM = pl.BlockSpec(memory_space=pltpu.SMEM)


def kernel(body, out_shape, operands, scalars=0, scratch=(), flops=0, mib=16, **static):
    return pl.pallas_call(
        functools.partial(body, **static),
        out_shape=out_shape,
        in_specs=[SMEM] * scalars + [VMEM] * (len(operands) - scalars),
        out_specs=jax.tree.map(lambda unused: VMEM, out_shape),
        scratch_shapes=scratch,
        compiler_params=pltpu.CompilerParams(vmem_limit_bytes=mib << 20),
        cost_estimate=pl.CostEstimate(
            flops=flops, bytes_accessed=1 << 20, transcendentals=0
        ),
    )(*operands)


def on_device(tokens, w_query, key_value_weight, w_out, doc_lengths):
    z, x, y, core = (lax.axis_index(name) for name in ("z", "x", "y", "core"))
    depth = lax.axis_size("z")
    rows, features = tokens.shape
    stripes = PAIR * PAIR
    block = w_query.shape[0]
    line = depth == 4

    def exchange(part):
        other = lax.ppermute(part, ("core", "x"), [(1, 2), (2, 1)])
        return jnp.where(x == core, part, other)

    def near_of(part):
        near = lax.ppermute(part, "z", BESIDE)
        even = z % 2 == 0
        return jnp.stack([jnp.where(even, part, near), jnp.where(even, near, part)])

    def middle_of(pair):
        return lax.ppermute(pair, "z", [(1, 2), (2, 1)])

    def far_of(middle):
        end = lax.ppermute(middle, "z", [(1, 0), (2, 3)])
        return jnp.where((z == 1) | (z == 2), middle, end)

    def gathered(part):
        held = lax.all_gather(part, "z", axis=0, tiled=False)
        return held, lax.ppermute(held, "core", SWAP)

    spots = jnp.arange(PAIR * depth, dtype=jnp.int32)
    flip = z // 2 * 2 if line else 0
    spots = ((spots % depth) ^ flip) * PAIR + ((spots // depth) ^ core)
    cut = rows // 2
    normed = kernel(
        normalise,
        [jax.ShapeDtypeStruct((count, features), jnp.bfloat16) for count in (cut, rows - cut)],
        (spots, tokens),
        scalars=1,
        flops=1 << 30,
        block=block,
        aligned=block % HEAD_SIZE == 0,
    )
    if block % HEAD_SIZE:
        normed = [
            jnp.take(part.reshape(len(part), -1, block), spots, axis=1).reshape(part.shape)
            for part in normed
        ]
    by_y = [lax.ppermute(normed[i], "y", SWAP) for i in range(2)]
    by_x = [lax.ppermute(normed[i], "x", SWAP) for i in range(2)]
    by_both = [lax.ppermute(by_x[0], "y", SWAP), lax.ppermute(by_y[1], "x", SWAP)]
    block_input = (*normed, *by_y, *by_x, *by_both)
    stripe_index = jnp.arange(stripes, dtype=jnp.int32) ^ (x * PAIR + y)

    keyval_own = exchange(key_value_weight).reshape(block, -1)
    query_own = exchange(w_query)
    out_own = exchange(w_out)
    if line:
        pair = near_of(keyval_own)
        far = far_of(middle_of(pair))
        keyval_weights = [
            pair, far, lax.ppermute(pair, "core", SWAP), lax.ppermute(far, "core", SWAP)
        ]
        pairs = jnp.split(near_of(query_own), QUERY_CHUNKS, axis=2)
        query_weights = []
        for pair in pairs:
            far = far_of(middle_of(pair))
            query_weights.append([
                pair, far, lax.ppermute(pair, "core", SWAP), lax.ppermute(far, "core", SWAP)
            ])
    else:
        keyval_weights = gathered(keyval_own)
        query_weights = [gathered(part) for part in jnp.split(query_own, QUERY_CHUNKS, axis=1)]

    span = stripes * PAIR * rows
    planes = depth // 4 + 1
    positions = (
        z * span
        + (stripe_index[:, None] * PAIR + core) * rows
        + jnp.arange(rows, dtype=jnp.int32)[None, :]
    ).reshape(-1)
    starts = ranks_of(doc_lengths, positions)
    half = HEAD_SIZE // 2
    freqs = jnp.power(rope_base, -2.0 * jnp.arange(half, dtype=jnp.float32) / HEAD_SIZE)
    angle = (positions - starts).astype(jnp.float32)[:, None] * freqs[None, :]
    cosine, sine = jnp.cos(angle), jnp.sin(angle)
    cosine = jnp.concatenate([cosine, cosine], axis=1)
    sine = jnp.concatenate([-sine, sine], axis=1)
    low = starts - (z - (planes - 1)) * span
    low = jnp.broadcast_to(low[:, None], (low.shape[0], HEAD_SIZE))

    count = stripes * rows
    keyval = kernel(
        keys_values,
        jax.ShapeDtypeStruct((count, 2 * HEAD_SIZE), jnp.bfloat16),
        (cosine, sine, *block_input, *keyval_weights),
        flops=4 * count * features * HEAD_SIZE,
        held=len(block_input),
    )
    held = []
    for distance in range(planes - 1, -1, -1):
        own = keyval
        if distance:
            steps = [(i, i + distance) for i in range(depth - distance)]
            own = lax.ppermute(keyval, "z", steps)
        held += [own, lax.ppermute(own, "core", SWAP)]

    scalars = jnp.arange(-1, stripes, dtype=jnp.int32)
    scalars = jnp.where(scalars < 0, core, scalars ^ (x * PAIR + y))
    mixed = []
    for weights in query_weights:
        columns = weights[0].shape[-1]
        mixed.append(
            kernel(
                attend,
                jax.ShapeDtypeStruct((count, columns), jnp.bfloat16),
                (scalars, cosine, sine, low, *block_input, *weights, *held),
                scalars=1,
                scratch=[pltpu.VMEM((count, columns), jnp.float32)]
                + [pltpu.VMEM((planes * span, HEAD_SIZE), jnp.bfloat16)] * 2,
                flops=2 * count * columns * (features + 2 * planes * span),
                mib=16 + 4 * planes,
                planes=planes,
                held=len(block_input),
                heads=columns // HEAD_SIZE,
                stripes=stripes,
                rows=rows,
            )
        )
    place = jnp.stack([core, z // 2 * 2]).astype(jnp.int32)

    width = w_out.shape[1] // OUT_CHUNKS
    per = w_out.shape[0]
    if line:
        halves = []
        near = lax.ppermute(out_own, "z", BESIDE)
        half = w_out.shape[1] // 2
        for at in (0, half):
            pair = (out_own[:, at : at + half], near[:, at : at + half])
            even = z % 2 == 0
            pair = [jnp.where(even, pair[0], pair[1]), jnp.where(even, pair[1], pair[0])]
            pair = lax.optimization_barrier(jnp.stack(pair))
            pair_c = lax.ppermute(pair, "core", SWAP)
            middle = middle_of(pair)
            cuts = [middle[:, :, at : at + width] for at in range(0, half, width)]
            halves.append((pair, pair_c, lax.optimization_barrier(cuts)))
    outs = []
    for chunk in range(OUT_CHUNKS):
        cols = slice(chunk * width, (chunk + 1) * width)
        axes = FIRST_SUM[chunk]
        if line:
            pair, pair_c, middle = halves[chunk * 2 // OUT_CHUNKS]
            inner = chunk % (OUT_CHUNKS // 2)
            far = far_of(middle[inner])
            far_c = lax.ppermute(far, "core", SWAP)
            shares = kernel(
                share_out,
                [jax.ShapeDtypeStruct((PAIR, rows, width // len(axes)), jnp.bfloat16)]
                * (2 * len(axes)),
                (place, *mixed, pair, far, pair_c, far_c),
                scalars=1,
                scratch=[pltpu.VMEM((2 * depth * per, width), jnp.bfloat16)],
                flops=2 * count * 2 * depth * per * width,
                parts=len(mixed),
                axes=axes,
                inner=inner * width,
            )
        else:
            mine, theirs = gathered(out_own[:, cols])
            weights = jnp.stack(
                [jnp.where(core == 0, mine, theirs), jnp.where(core == 0, theirs, mine)], axis=1
            ).reshape(2 * depth * per, width)
            share = jnp.dot(
                jnp.concatenate(mixed, axis=1), weights, preferred_element_type=jnp.float32
            ).astype(jnp.bfloat16)
            share = share.reshape(PAIR, PAIR, rows, len(axes), width // len(axes))
            shares = [
                share[:, i, :, part] if axis == "y" else share[i, :, :, part]
                for part, axis in enumerate(axes)
                for i in range(PAIR)
            ]
        for part, axis in enumerate(axes):
            kept, sent = shares[2 * part : 2 * part + 2]
            got = lax.ppermute(sent, axis, SWAP)
            kept = kept.astype(jnp.float32) + got.astype(jnp.float32)
            kept = kept.astype(jnp.bfloat16)
            other = "x" if axis == "y" else "y"
            outs += [kept, lax.ppermute(kept[1], other, SWAP)]
    return kernel(last_sum, jax.ShapeDtypeStruct((rows, w_out.shape[1]), jnp.bfloat16), outs)


def solution(mesh):
    groups, blocks = mesh.shape["heads"], mesh.shape["blk"]
    depth = blocks // PAIR
    fine = Mesh(
        mesh.devices.reshape(groups // PAIR, PAIR, depth, PAIR),
        ("y", "core", "z", "x"),
    )
    return jax.shard_map(
        on_device,
        mesh=fine,
        in_specs=(
            P(("z", "x", "y", "core"), None),
            P(("z", "x"), ("y", "core")),
            P(("z", "x"), None, ("y", "core")),
            P(("y", "core", "z", "x"), None),
            P(),
        ),
        out_specs=P(("z", "x", "y", "core"), None),
        check_vma=False,
    )
```
